512 devices in a mesh: row: 32 (over y_hi, z, core), col: 16 (over x, y_lo).
Axes of the slice: x: 4, y: 8 (y_hi: 2, y_lo: 4; y = y_hi * 4 + y_lo), z: 8, core: 2. Of those that a mesh axis runs over, the one named last changes fastest.
Arguments:
- embedding: bfloat16 [1024, 128], P('col'), may hold values from -6 to 6
- dilation: int32 [2], replicated, may hold values from 1 to 4, as said below
- kernel: bfloat16 [3, 3, 48, 128], replicated, may hold values from -0.1875 to 0.1875
- kernel_bias: float32 [48], replicated, may hold values from -3 to 3
- mixing: bfloat16 [5, 48], replicated, may hold values from -0.875 to 0.875
- mixing_bias: float32 [5], replicated, may hold values from -3 to 3
- cotangent: bfloat16 [5, 1024, 1024], P(None, 'row', 'col'), may hold values from -0.375 to 0.375
Outputs:
- contact: float32 [5, 1024, 1024], P(None, 'row', 'col')
- embedding_grad: float32 [1024, 128], P('col')
- kernel_grad: float32 [3, 3, 48, 128], replicated
The draws below stay inside these ranges and needn't reach their ends.
Inputs may be any that keep to these rules, and one draw needn't show every extreme that they name: `dilation`: the larger of the two rates is exactly 4.
All inputs are finite; a program needn't handle non-finite values.
Results may differ from the reference program's by a relative error of at most 0.019.
The reference program's roundings to bfloat16 on the way count: a program that leaves them out, or rounds other values in their place, can miss the bound.
Values may be sent and summed in bfloat16 or wider, within the bound.
A program may use at most 64 MiB of HBM per device.

```python
import jax
import jax.numpy as jnp
from jax import lax

C = 128
F = 48
NT = 5
DMAX = 4
BINS = 1024
RB = 32
N_ROW = 32


def draw_dilation(key, part):
    first_key, second_key = jax.random.split(jax.random.fold_in(key, 11))
    larger_slot = jax.random.randint(first_key, (), 0, 2)
    other_rate = jax.random.randint(second_key, (), 1, DMAX + 1)
    slot_index = jnp.arange(2)
    return jnp.where(slot_index == larger_slot, DMAX, other_rate).astype(jnp.int32)


def block_scale(stream_key, shape, shards, low, high):
    factor_of, own = 1.0, jax.random.fold_in(stream_key, 6)
    for dim, shards_of in shards:
        steps = jnp.exp(jax.random.uniform(jax.random.fold_in(own, dim), (shards_of,), jnp.float32, low / len(shards), high / len(shards)))
        factor_of = factor_of * jnp.repeat(steps, shape[dim] // shards_of).reshape([-1 if axis == dim else 1 for axis in range(len(shape))])
    return factor_of


def normal_values(own_key, dims, spread, most, shards=(), kind=jnp.bfloat16):
    array = spread * jax.random.normal(own_key, dims, jnp.float32)
    if shards:
        array = array * block_scale(own_key, dims, shards, -0.22, 0.18)
    return jnp.clip(array, -most, most).astype(kind)


def setup_inputs(seed: int = 0) -> dict:
    splits = jax.random.split(jax.random.key(seed), 8)
    return {
        "embedding": normal_values(splits[0], (BINS, C), 1.0, 6.0, ((0, 16),)),
        "dilation": draw_dilation(jax.random.fold_in(splits[7], 71), 0),
        "kernel": normal_values(splits[2], (3, 3, F, C), (9 * C) ** -0.5, 0.1875),
        "kernel_bias": normal_values(splits[3], (F,), 0.5, 3.0, (), jnp.float32),
        "mixing": normal_values(splits[4], (NT, F), F ** -0.5, 0.875),
        "mixing_bias": normal_values(splits[5], (NT,), 0.5, 3.0, (), jnp.float32),
        "cotangent": normal_values(splits[6], (NT, BINS, BINS), 0.0625, 0.375, ((1, 32), (2, 16))),
    }


def tap_list():
    return [(tap_row, tap_col) for tap_row in (-1, 0, 1) for tap_col in (-1, 0, 1)]


def tap_anchor(tap_row, tap_col, row_rate, col_rate, mirrored):
    if mirrored:
        return DMAX + tap_col * col_rate, DMAX + tap_row * row_rate
    return DMAX + tap_row * row_rate, DMAX + tap_col * col_rate


def narrow(values):
    return lax.optimization_barrier(values.astype(jnp.bfloat16)).astype(jnp.float32)


def add_into(target, position, update):
    current = lax.dynamic_slice_in_dim(target, position, update.shape[0], 0)
    return lax.dynamic_update_slice_in_dim(target, current + update, position, 0)


def reference(embedding, dilation, kernel, kernel_bias, mixing, mixing_bias, cotangent):
    highest = lax.Precision.HIGHEST
    row_rate = dilation[0].astype(jnp.int32)
    col_rate = dilation[1].astype(jnp.int32)
    padded_len = BINS + 2 * DMAX
    padded = jnp.pad(embedding.astype(jnp.float32), ((DMAX, DMAX), (0, 0)))
    places = jnp.arange(padded_len, dtype=jnp.int32) - DMAX
    inside = ((places >= 0) & (places < BINS)).astype(jnp.float32)
    weights = kernel.astype(jnp.float32)
    mix_weights = mixing.astype(jnp.float32)
    zero_index = jnp.zeros((), jnp.int32)

    def block_step(running_sums, block_index):
        kernel_acc, row_acc, col_acc = running_sums
        block_start = block_index * RB
        row_values = lax.dynamic_slice_in_dim(padded, block_start, RB + 2 * DMAX, 0)
        row_inside = lax.dynamic_slice_in_dim(inside, block_start, RB + 2 * DMAX, 0)
        pairs = narrow(0.5 * (row_values[:, None, :] + padded[None, :, :]))
        pairs = pairs * (row_inside[:, None] * inside[None, :])[:, :, None]

        def slicer(tap_row, tap_col, mirrored):
            anchor = tap_anchor(tap_row, tap_col, row_rate, col_rate, mirrored)
            return lax.dynamic_slice(pairs, (anchor[0], anchor[1], zero_index), (RB, BINS, C))

        def convolve(mirrored):
            running = jnp.zeros((F, RB, BINS), jnp.float32)
            for tap_row, tap_col in tap_list():
                tap_piece = slicer(tap_row, tap_col, mirrored)
                running = running + jnp.einsum("ijc,fc->fij", tap_piece, weights[tap_row + 1, tap_col + 1], precision=highest)
            return running + kernel_bias[:, None, None]

        direct = convolve(False)
        mirror = convolve(True)
        direct_act = narrow(jax.nn.relu(direct))
        mirror_act = narrow(jax.nn.relu(mirror))

        def mix_map(activation):
            return jnp.einsum("tf,fij->tij", mix_weights, activation, precision=highest) + mixing_bias[:, None, None]

        contact_block = 0.5 * mix_map(direct_act) + 0.5 * mix_map(mirror_act)
        target = lax.dynamic_slice_in_dim(cotangent, block_start, RB, 1).astype(jnp.float32)
        guide_grad = narrow(0.5 * jnp.einsum("tf,tij->fij", mix_weights, target, precision=highest))
        grad_direct = jnp.where(direct > 0, guide_grad, jnp.zeros_like(guide_grad))
        grad_mirror = jnp.where(mirror > 0, guide_grad, jnp.zeros_like(guide_grad))

        updates = []
        for tap_row, tap_col in tap_list():
            tap_term = jnp.einsum("fij,ijc->fc", grad_direct, slicer(tap_row, tap_col, False), precision=highest)
            tap_term = tap_term + jnp.einsum("fij,ijc->fc", grad_mirror, slicer(tap_row, tap_col, True), precision=highest)
            updates.append(tap_term)
        kernel_acc = kernel_acc + jnp.stack(updates).reshape(3, 3, F, C)

        def col_mask(shift):
            return lax.dynamic_slice_in_dim(inside, DMAX + shift, BINS, 0)

        def row_mask(shift):
            return lax.dynamic_slice_in_dim(row_inside, DMAX + shift, RB, 0)

        direct_rows = [jnp.einsum("fij,j->fi", grad_direct, col_mask(tap_step * col_rate), precision=highest) for tap_step in (-1, 0, 1)]
        direct_cols = [jnp.einsum("fij,i->fj", grad_direct, row_mask(tap_step * row_rate), precision=highest) for tap_step in (-1, 0, 1)]
        mirror_rows = [jnp.einsum("fij,j->fi", grad_mirror, col_mask(tap_step * row_rate), precision=highest) for tap_step in (-1, 0, 1)]
        mirror_cols = [jnp.einsum("fij,i->fj", grad_mirror, row_mask(tap_step * col_rate), precision=highest) for tap_step in (-1, 0, 1)]
        for tap_row, tap_col in tap_list():
            tap_weight = weights[tap_row + 1, tap_col + 1]
            row_acc = add_into(row_acc, block_start + DMAX + tap_row * row_rate, jnp.einsum("fi,fc->ic", direct_rows[tap_col + 1], tap_weight, precision=highest))
            row_acc = add_into(row_acc, block_start + DMAX + tap_col * col_rate, jnp.einsum("fi,fc->ic", mirror_rows[tap_row + 1], tap_weight, precision=highest))
            col_acc = add_into(col_acc, DMAX + tap_col * col_rate, jnp.einsum("fj,fc->jc", direct_cols[tap_row + 1], tap_weight, precision=highest))
            col_acc = add_into(col_acc, DMAX + tap_row * row_rate, jnp.einsum("fj,fc->jc", mirror_cols[tap_col + 1], tap_weight, precision=highest))
        return (kernel_acc, row_acc, col_acc), contact_block

    initial = (jnp.zeros((3, 3, F, C), jnp.float32), jnp.zeros((padded_len, C), jnp.float32), jnp.zeros((padded_len, C), jnp.float32))
    finals, blocks = lax.scan(block_step, initial, jnp.arange(N_ROW, dtype=jnp.int32))
    kernel_grad, row_acc, col_acc = finals
    contact = jnp.transpose(blocks, (1, 0, 2, 3)).reshape(NT, BINS, BINS)
    embedding_grad = 0.5 * row_acc[DMAX:DMAX + BINS] + 0.5 * col_acc[DMAX:DMAX + BINS]
    return contact, embedding_grad, kernel_grad
```

```python
import functools

import jax
import jax.numpy as jnp
from jax import lax
from jax.experimental import pallas as pl
from jax.experimental.pallas import tpu as pltpu
from jax.sharding import PartitionSpec as P

MESH = pl.DeviceIdType.MESH
DMAX = 4
TILE = 16
LANES = 128
MIRROR = 64
TAPS = [(a, b) for a in range(3) for b in range(3)]
VM = pl.BlockSpec(memory_space=pltpu.VMEM)
SM = pl.BlockSpec(memory_space=pltpu.SMEM)


def f32(value):
    return value.astype(jnp.float32)


def b16(value):
    return value.astype(jnp.bfloat16)


def dot(a, b, dims):
    return lax.dot_general(a, b, (dims, ((), ())), preferred_element_type=jnp.float32)


def load_weights(kern, bias, mix, wconv, wall, bias_row, mix_rows):
    filters = kern.shape[2]
    wconv[...] = jnp.zeros_like(wconv)
    wall[...] = jnp.zeros_like(wall)
    bias_row[...] = jnp.zeros_like(bias_row)
    mix_rows[...] = jnp.zeros_like(mix_rows)
    for at in (0, MIRROR):
        bias_row[:, at : at + filters] = bias[...]
        mix_rows[0 : mix.shape[0], at : at + filters] = f32(mix[...])
    for n, (a, b) in enumerate(TAPS):
        tap = kern[a, b]
        wconv[0:filters, n * LANES : (n + 1) * LANES] = tap
        wconv[MIRROR : MIRROR + filters, (9 + n) * LANES : (10 + n) * LANES] = tap
        wall[b * LANES : b * LANES + filters, a * LANES : (a + 1) * LANES] = tap
        wall[a * LANES + MIRROR : a * LANES + MIRROR + filters, (3 + b) * LANES : (4 + b) * LANES] = tap


def compute(
    dil, erow, ecol, cot, mixb, contact, send,
    wconv, wall, bias_row, mix_rows,
    er, ec, xr, xc, mr, mc, cotf, lhs, sums, sums_c, prow, pcol,
    row_index, col_index, bins, half, tiles_per_owner, owners,
):
    rows = contact.shape[1]
    cols = contact.shape[2]
    row_rate = dil[0]
    col_rate = dil[1]
    shifts = [-row_rate, 0, row_rate, -col_rate, 0, col_rate]
    row_start = row_index * rows
    col_start = col_index * cols

    er[...] = 0.5 * f32(erow[...])
    ec[...] = 0.5 * f32(ecol[...])
    lane_r = lax.broadcasted_iota(jnp.int32, (rows, LANES), 1)
    lane_c = lax.broadcasted_iota(jnp.int32, (cols, LANES), 1)
    row_at = lax.broadcasted_iota(jnp.int32, (rows, LANES), 0) + row_start
    col_at = lax.broadcasted_iota(jnp.int32, (cols, LANES), 0) + col_start

    def inside(place):
        return jnp.where((place >= 0) & (place < bins), 1.0, 0.0)

    for q, shift in enumerate(shifts):
        xr[q] = er[pl.ds(TILE + shift, rows), :]
        xc[q] = b16(ec[pl.ds(TILE + shift, cols), :])
        mr[q] = inside(row_at + shift)
        mc[q] = b16(inside(col_at + shift))
    sum_rm = [
        inside(row_at + jnp.where(lane_r < MIRROR, t * row_rate, t * col_rate)) for t in (-1, 1)
    ]
    sum_cm = [
        inside(col_at + jnp.where(lane_c < MIRROR, t * col_rate, t * row_rate)) for t in (-1, 1)
    ]
    for t in range(2):
        mr[6 + t] = sum_rm[t]
    cotf[...] = f32(cot[...])
    sums_c[...] = jnp.zeros_like(sums_c)
    mix16 = b16(mix_rows[...])

    group = 8

    @pl.loop(0, rows // group)
    def _(chunk):
        base = chunk * group
        for ii in range(group):
            i = base + ii
            row16 = [b16(jnp.broadcast_to(xr[q, pl.ds(i, 1), :], (TILE, LANES))) for q in range(6)]
            rmask = [b16(jnp.broadcast_to(mr[q, pl.ds(i, 1), :], (TILE, LANES))) for q in range(6)]
            for n in range(18):
                a, b = TAPS[n % 9]
                p, q = (a, 3 + b) if n < 9 else (3 + b, a)
                for s in range(cols // TILE):
                    value = (row16[p] + xc[q, s * TILE : (s + 1) * TILE, :]) * mc[
                        q, s * TILE : (s + 1) * TILE, :
                    ]
                    lhs[ii * cols + s * TILE : ii * cols + (s + 1) * TILE, n * LANES : (n + 1) * LANES] = (
                        value * rmask[p]
                    )
        conv = dot(lhs[...], wconv[...], ((1,), (1,))) + bias_row[...]
        on = conv > 0
        act = b16(jnp.maximum(conv, 0.0))
        mixed = 0.5 * dot(mix16, act, ((1,), (1,)))
        guide = []
        for ii in range(group):
            piece = b16(cotf[:, base + ii, :])
            guide.append(dot(piece, mix16[0:8], ((0,), (0,))))
        guide = f32(b16(0.5 * jnp.concatenate(guide, axis=0)))
        grad = jnp.where(on, guide, 0.0)
        row_sums = [[], [], []]
        maps = []
        for ii in range(group):
            i = base + ii
            g = grad[ii * cols : (ii + 1) * cols]
            maps.append(mixed[0:5, ii * cols : (ii + 1) * cols] + mixb[...])
            for t in range(3):
                gr = g if t == 1 else g * sum_cm[t // 2]
                row_sums[t].append(jnp.sum(gr, axis=0, keepdims=True))
                gc = g if t == 1 else g * jnp.broadcast_to(mr[6 + t // 2, pl.ds(i, 1), :], g.shape)
                sums_c[:, t * LANES : (t + 1) * LANES] += gc
        at = pl.multiple_of(base, group)
        contact[:, pl.ds(at, group), :] = jnp.stack(maps, axis=1)
        for t in range(3):
            sums[pl.ds(at, group), t * LANES : (t + 1) * LANES] = jnp.concatenate(row_sums[t], axis=0)

    for t in range(3):
        block = sums_c[:, t * LANES : (t + 1) * LANES]
        sums[rows : rows + cols, t * LANES : (t + 1) * LANES] = pltpu.roll(block, MIRROR, 1)
    stacked = b16(sums[...])
    emb = 0.5 * dot(stacked, wall[...], ((1,), (0,)))
    prow[...] = jnp.zeros_like(prow)
    pcol[...] = jnp.zeros_like(pcol)
    for q in range(6):
        part = emb[:, q * LANES : (q + 1) * LANES]
        prow[q, 24 : 24 + rows] = part[0:rows]
        pcol[q, 24 : 24 + cols] = part[rows : rows + cols]
    row_grad = sum(prow[q, pl.ds(8 - shifts[q], rows + 2 * TILE), :] for q in range(6))
    col_grad = sum(pcol[q, pl.ds(8 - shifts[q], cols + 2 * TILE), :] for q in range(6))

    kernel_tiles = tiles_per_owner * owners
    x = [jnp.concatenate([b16(xr[q]), xc[q]], axis=0) for q in range(6)]
    wide = dot(stacked, jnp.concatenate(x, axis=1), ((0,), (0,)))
    filters = 48
    pieces = []
    for a, b in TAPS:
        tap = (
            wide[b * LANES : b * LANES + filters, a * LANES : (a + 1) * LANES]
            + wide[a * LANES + MIRROR : a * LANES + MIRROR + filters, (3 + b) * LANES : (4 + b) * LANES]
        )
        pieces += [tap[s * TILE : (s + 1) * TILE] for s in range(filters // TILE)]
    zero = jnp.zeros((TILE, LANES), jnp.bfloat16)
    for k in range(2 * kernel_tiles):
        send[k % 2, k // 2] = b16(pieces[k]) if k < len(pieces) else zero
    for k in range(6):
        send[k // 3, kernel_tiles + k % 3] = b16(col_grad[k * TILE : (k + 1) * TILE])
        send[k // 3, kernel_tiles + 3 + k % 3] = zero
    for k in range(4):
        value = b16(row_grad[k * TILE : (k + 1) * TILE])

        @pl.when(half == 0)
        def _():
            send[k // 3, kernel_tiles + 3 + k % 3] = value

        @pl.when(half == 1)
        def _():
            send[(k + 2) // 3, kernel_tiles + 3 + (k + 2) % 3] = value


def compute_kernel(owners, tiles_per_owner, bins, dil, erow, ecol, kern, bias, mix, mixb, cot, contact, send, *scratch):
    row_index = lax.axis_index("row")
    col_index = lax.axis_index("col")
    load_weights(kern, bias, mix, *scratch[:4])
    compute(
        dil, erow, ecol, cot, mixb, contact, send, *scratch,
        row_index, col_index, bins, lax.rem(row_index, 2), tiles_per_owner, owners,
    )


def compute_scratch(rows, cols, channels):
    return [
        pltpu.VMEM((LANES, 18 * LANES), jnp.bfloat16),
        pltpu.VMEM((3 * LANES, 6 * LANES), jnp.bfloat16),
        pltpu.VMEM((1, LANES), jnp.float32),
        pltpu.VMEM((8, LANES), jnp.float32),
        pltpu.VMEM((rows + 2 * TILE, LANES), jnp.float32),
        pltpu.VMEM((cols + 2 * TILE, LANES), jnp.float32),
        pltpu.VMEM((6, rows, LANES), jnp.float32),
        pltpu.VMEM((6, cols, LANES), jnp.bfloat16),
        pltpu.VMEM((8, rows, LANES), jnp.float32),
        pltpu.VMEM((6, cols, LANES), jnp.bfloat16),
        pltpu.VMEM((8, rows, cols), jnp.float32),
        pltpu.VMEM((8 * cols, 18 * LANES), jnp.bfloat16),
        pltpu.VMEM((rows + cols, 3 * LANES), jnp.float32),
        pltpu.VMEM((cols, 3 * LANES), jnp.float32),
        pltpu.VMEM((6, rows + 48, LANES), jnp.float32),
        pltpu.VMEM((6, cols + 48, LANES), jnp.float32),
    ]


class Place:
    def __init__(self, n_row, n_col):
        self.n_col = n_col
        self.n_z = n_row // 4
        self.row = lax.axis_index("row")
        self.col = lax.axis_index("col")
        self.half = lax.rem(self.row, 2)
        self.chip = self.row // 2
        self.z = lax.rem(self.chip, self.n_z)
        self.partner = self.row + 1 - 2 * self.half
        self.far = lax.rem(self.row + n_row // 2, n_row)

    def z_peer(self, z):
        return self.row + 2 * (z - self.z)


def enter(place, barrier):
    count = 0

    def greet(row, col):
        pl.semaphore_signal(barrier, inc=1, device_id=(row, col), device_id_type=MESH)

    greet(place.partner, place.col)
    greet(place.far, place.col)
    count += 2
    for d in range(1, place.n_z):
        greet(place.z_peer(lax.rem(place.z + d, place.n_z)), place.col)
        count += 1
    for d in range(1, place.n_col):
        greet(place.row, lax.rem(place.col + d, place.n_col))
        count += 1
    for d in (1, place.n_col - 1):
        greet(place.partner, lax.rem(place.col + d, place.n_col))
        count += 1
    return count


def remote(src, dst, send_sem, recv_sem, row, col):
    return pltpu.make_async_remote_copy(
        src_ref=src, dst_ref=dst, send_sem=send_sem, recv_sem=recv_sem, device_id=(row, col), device_id_type=MESH
    )


def total(ref, count):
    value = f32(ref[0])
    for k in range(1, count):
        value = value + f32(ref[k])
    return value


def reduce_all(
    place, owners, per_owner, send, emb_out, kernel_out,
    core_in, own, r_kernel, r_row, p_kernel, p_emb, y_kernel, y_emb,
    z_kernel, z_emb, full, emb_all, margins,
    core_s, kern_s, row_s, y_s, zk_s, ze_s, ag_s, agc_s, fin_s,
):
    n_col, n_z = place.n_col, place.n_z
    row, col, half = place.row, place.col, place.half
    kt = per_owner * owners

    swap = remote(send.at[1 - half], core_in, core_s.at[0], core_s.at[1], place.partner, col)
    swap.start()
    swap.wait()
    own[...] = b16(f32(send[half]) + f32(core_in[...]))

    def kernel_copy(src, dst):
        return remote(
            own.at[pl.ds(dst * per_owner, per_owner)],
            r_kernel.at[src],
            kern_s.at[0, dst],
            kern_s.at[1, src],
            row,
            dst,
        )

    for dst in range(owners):

        @pl.when(dst != col)
        def _():
            kernel_copy(col, dst).start()

    def row_copy(src):
        return remote(own.at[pl.ds(kt + 3, 3)], r_row.at[src], row_s.at[n_col], row_s.at[src], row, place.chip)

    @pl.when(col != place.chip)
    def _():
        row_copy(col).start()

    def far_copy(n, src, dst):
        return remote(src, dst, y_s.at[0, n], y_s.at[1, n], place.far, col)

    def z_copy(sems, buf, src, dst):
        return remote(buf.at[src], buf.at[src], sems.at[0, dst], sems.at[1, src], place.z_peer(dst), col)

    @pl.when(col < owners)
    def _():
        r_kernel[col] = own[pl.ds(col * per_owner, per_owner)]
        for src in range(n_col):

            @pl.when(src != col)
            def _():
                kernel_copy(src, col).wait_recv()

        p_kernel[...] = b16(total(r_kernel, n_col))
        far_copy(0, p_kernel, y_kernel).start()

    mine = f32(own[kt : kt + 3])
    p_emb[...] = b16(mine)

    @pl.when(col == place.chip)
    def _():
        r_row[col] = own[kt + 3 : kt + 6]
        for src in range(n_col):

            @pl.when(src != col)
            def _():
                row_copy(src).wait_recv()

        p_emb[...] = b16(mine + total(r_row, n_col))

    far_copy(1, p_emb, y_emb).start()

    @pl.when(col < owners)
    def _():
        far_copy(0, p_kernel, y_kernel).wait()
        z_kernel[place.z] = b16(f32(p_kernel[...]) + f32(y_kernel[...]))
        for dst in range(n_z):

            @pl.when(dst != place.z)
            def _():
                z_copy(zk_s, z_kernel, place.z, dst).start()

    far_copy(1, p_emb, y_emb).wait()
    z_emb[place.z] = b16(f32(p_emb[...]) + f32(y_emb[...]))
    for dst in range(n_z):

        @pl.when(dst != place.z)
        def _():
            z_copy(ze_s, z_emb, place.z, dst).start()

    def gather_copy(src, dst):
        return remote(full.at[half, src], full.at[half, src], ag_s.at[0, dst], ag_s.at[1, src], row, dst)

    @pl.when(col < owners)
    def _():
        for src in range(n_z):

            @pl.when(src != place.z)
            def _():
                z_copy(zk_s, z_kernel, src, place.z).wait_recv()

        full[half, col] = b16(total(z_kernel, n_z))
        for dst in range(n_col):

            @pl.when(dst != col)
            def _():
                gather_copy(col, dst).start()

    for src in range(n_z):

        @pl.when(src != place.z)
        def _():
            z_copy(ze_s, z_emb, src, place.z).wait_recv()

    emb_all[half] = b16(total(z_emb, n_z))
    emb_swap = remote(emb_all.at[half], emb_all.at[half], fin_s.at[0, 0], fin_s.at[1, 0], place.partner, col)
    emb_swap.start()
    to = col - 1 + 2 * half
    exists = (to >= 0) & (to < n_col)
    came = col + 1 - 2 * half
    came_ok = (came >= 0) & (came < n_col)
    other = col - 1 + 2 * half
    other_ok = (other >= 0) & (other < n_col)

    def margin_copy(n, device_row):
        return remote(
            emb_all.at[half, 2 * half], margins.at[half], fin_s.at[0, 1 + n], fin_s.at[1, 1 + n], device_row, to
        )

    def margin_in(n, slot):
        return remote(
            emb_all.at[half, 2 * half], margins.at[slot], fin_s.at[0, 1 + n], fin_s.at[1, 1 + n], row, col
        )

    @pl.when(exists)
    def _():
        margin_copy(0, row).start()
        margin_copy(1, place.partner).start()

    emb_swap.wait()

    @pl.when(came_ok)
    def _():
        margin_in(0, half).wait_recv()

    @pl.when(other_ok)
    def _():
        margin_in(1, 1 - half).wait_recv()

    main = [f32(emb_all[0, 1]), f32(emb_all[0, 2]), f32(emb_all[1, 0]), f32(emb_all[1, 1])]
    emb_out[0:TILE] = main[0] + f32(margins[1])
    emb_out[TILE : 2 * TILE] = main[1]
    emb_out[2 * TILE : 3 * TILE] = main[2]
    emb_out[3 * TILE : 4 * TILE] = main[3] + f32(margins[0])

    for src in range(owners):

        @pl.when(src != col)
        def _():
            gather_copy(src, col).wait_recv()

    share = remote(full.at[half], full.at[half], agc_s.at[0], agc_s.at[1], place.partner, col)
    share.start()
    share.wait()
    count = kernel_out.shape[0]
    for k in range(count):
        kernel_out[k] = f32(full[k % 2, k // (2 * per_owner), (k // 2) % per_owner])

    for dst in range(owners):

        @pl.when(dst != col)
        def _():
            kernel_copy(col, dst).wait_send()

    @pl.when(col != place.chip)
    def _():
        row_copy(col).wait_send()

    for dst in range(n_z):

        @pl.when((dst != place.z) & (col < owners))
        def _():
            z_copy(zk_s, z_kernel, place.z, dst).wait_send()

        @pl.when(dst != place.z)
        def _():
            z_copy(ze_s, z_emb, place.z, dst).wait_send()

    @pl.when(col < owners)
    def _():
        for dst in range(n_col):

            @pl.when(dst != col)
            def _():
                gather_copy(col, dst).wait_send()

    @pl.when(exists)
    def _():
        margin_copy(0, row).wait_send()
        margin_copy(1, place.partner).wait_send()


def reduce_kernel(n_row, n_col, owners, per_owner, send, emb_out, kernel_out, *scratch):
    place = Place(n_row, n_col)
    margins = scratch[12]
    margins[...] = jnp.zeros_like(margins)
    barrier = pltpu.get_barrier_semaphore()
    pl.semaphore_wait(barrier, enter(place, barrier))
    reduce_all(place, owners, per_owner, send, emb_out, kernel_out, *scratch)


def reduce_scratch(n_row, n_col, owners, per_owner):
    n_z = n_row // 4
    kt = owners * per_owner

    def tiles(*lead):
        return pltpu.VMEM((*lead, TILE, LANES), jnp.bfloat16)

    return [
        tiles(kt + 6), tiles(kt + 6), tiles(n_col, per_owner), tiles(n_col, 3),
        tiles(per_owner), tiles(3), tiles(per_owner), tiles(3),
        tiles(n_z, per_owner), tiles(n_z, 3), tiles(2, owners, per_owner), tiles(2, 3), tiles(2),
        pltpu.SemaphoreType.DMA((2,)),
        pltpu.SemaphoreType.DMA((2, n_col)),
        pltpu.SemaphoreType.DMA((n_col + 1,)),
        pltpu.SemaphoreType.DMA((2, 2)),
        pltpu.SemaphoreType.DMA((2, n_z)),
        pltpu.SemaphoreType.DMA((2, n_z)),
        pltpu.SemaphoreType.DMA((2, n_col)),
        pltpu.SemaphoreType.DMA((2,)),
        pltpu.SemaphoreType.DMA((2, 3)),
    ]


def per_device(n_row, n_col, embedding, dilation, kernel, kernel_bias, mixing, mixing_bias, cotangent):
    channels = embedding.shape[1]
    filters = kernel.shape[2]
    maps, rows, cols = cotangent.shape
    bins = cols * n_col
    count = 9 * filters // TILE
    per_owner = -(-count // (2 * n_col))
    owners = -(-count // (2 * per_owner))
    row_start = lax.axis_index("row") * rows
    col_start = lax.axis_index("col") * cols
    tiles = lax.all_to_all(
        jnp.broadcast_to(embedding[None], (n_col, *embedding.shape)), "col", 0, 0, tiled=True
    ).reshape(bins, channels)
    padded = jnp.pad(tiles, ((TILE, TILE), (0, 0)))
    erow = lax.dynamic_slice_in_dim(padded, row_start, rows + 2 * TILE, 0)
    ecol = lax.dynamic_slice_in_dim(padded, col_start, cols + 2 * TILE, 0)
    cot8 = jnp.pad(cotangent, ((0, 8 - maps), (0, 0), (0, 0)))
    contact, send = pl.pallas_call(
        functools.partial(compute_kernel, owners, per_owner, bins),
        out_shape=[
            jax.ShapeDtypeStruct((maps, rows, cols), jnp.float32),
            jax.ShapeDtypeStruct((2, owners * per_owner + 6, TILE, LANES), jnp.bfloat16),
        ],
        in_specs=[SM, VM, VM, VM, VM, VM, VM, VM],
        out_specs=[VM, VM],
        scratch_shapes=compute_scratch(rows, cols, channels),
    )(dilation, erow, ecol, kernel, kernel_bias[None], mixing, mixing_bias[:, None], cot8)
    emb, grad = pl.pallas_call(
        functools.partial(reduce_kernel, n_row, n_col, owners, per_owner),
        out_shape=[
            jax.ShapeDtypeStruct((cols, channels), jnp.float32),
            jax.ShapeDtypeStruct((count, TILE, channels), jnp.float32),
        ],
        in_specs=[VM],
        out_specs=[VM, VM],
        scratch_shapes=reduce_scratch(n_row, n_col, owners, per_owner),
        compiler_params=pltpu.CompilerParams(collective_id=0, has_side_effects=True),
    )(send)
    return contact, emb, grad.reshape(3, 3, filters, channels)


def solution(mesh):
    return jax.shard_map(
        functools.partial(per_device, mesh.shape["row"], mesh.shape["col"]),
        mesh=mesh,
        in_specs=(P("col", None), P(), P(), P(), P(), P(), P(None, "row", "col")),
        out_specs=(P(None, "row", "col"), P("col", None), P()),
        check_vma=False,
    )
```

```python
import functools

import jax
import jax.numpy as jnp
from jax import lax
from jax.experimental import pallas as pl
from jax.experimental.pallas import tpu as pltpu
from jax.sharding import PartitionSpec as P

MESH = pl.DeviceIdType.MESH
DMAX = 4
TILE = 16
LANES = 128
MIRROR = 64
GROUP = 8
TAPS = [(a, b) for a in range(3) for b in range(3)]
VM = pl.BlockSpec(memory_space=pltpu.VMEM)
SM = pl.BlockSpec(memory_space=pltpu.SMEM)


def f32(value):
    return value.astype(jnp.float32)


def b16(value):
    return value.astype(jnp.bfloat16)


def dot(a, b, dims):
    return lax.dot_general(a, b, (dims, ((), ())), preferred_element_type=jnp.float32)


def load_weights(kern, bias, mix, wconv, wall, bias_row, mix_rows):
    filters = kern.shape[2]
    wconv[...] = jnp.zeros_like(wconv)
    wall[...] = jnp.zeros_like(wall)
    bias_row[...] = jnp.zeros_like(bias_row)
    mix_rows[...] = jnp.zeros_like(mix_rows)
    for at in (0, MIRROR):
        bias_row[:, at : at + filters] = bias[...]
        mix_rows[0 : mix.shape[0], at : at + filters] = f32(mix[...])
    for n, (a, b) in enumerate(TAPS):
        tap = kern[a, b]
        wconv[0:filters, n * LANES : (n + 1) * LANES] = tap
        wconv[MIRROR : MIRROR + filters, (9 + n) * LANES : (10 + n) * LANES] = tap
        wall[b * LANES : b * LANES + filters, a * LANES : (a + 1) * LANES] = tap
        wall[a * LANES + MIRROR : a * LANES + MIRROR + filters, (3 + b) * LANES : (4 + b) * LANES] = tap


def shift_list(dil):
    return [-dil[0], 0, dil[0], -dil[1], 0, dil[1]]


def prepare(dil, place, cot, mr, mc, sm, cotf, mix_rows, guide, rows, cols, bins):
    row_rate, col_rate = dil[0], dil[1]
    lane_r = lax.broadcasted_iota(jnp.int32, (rows, LANES), 1)
    lane_c = lax.broadcasted_iota(jnp.int32, (cols, LANES), 1)
    row_at = lax.broadcasted_iota(jnp.int32, (rows, LANES), 0) + place.row * rows
    col_at = lax.broadcasted_iota(jnp.int32, (cols, LANES), 0) + place.col * cols

    def inside(at):
        return jnp.where((at >= 0) & (at < bins), 1.0, 0.0)

    for q, shift in enumerate(shift_list(dil)):
        mr[q] = inside(row_at + shift)
        mc[q] = b16(inside(col_at + shift))
    for n, t in enumerate((-1, 1)):
        mr[6 + n] = inside(row_at + jnp.where(lane_r < MIRROR, t * row_rate, t * col_rate))
        sm[n] = inside(col_at + jnp.where(lane_c < MIRROR, t * col_rate, t * row_rate))
    cotf[...] = f32(cot[...])
    mix16 = b16(mix_rows[...])
    for i in range(rows):
        guide[i * cols : (i + 1) * cols] = b16(0.5 * dot(b16(cotf[:, i, :]), mix16[0 : cotf.shape[0]], ((0,), (0,))))


def convolve(dil, erow, ecol, wconv, bias_row, er, ec, xr, xc, mr, mc, sm, lhs, guide, acts, sums, rows, cols):
    shifts = shift_list(dil)
    for k in range(erow.shape[0]):
        er[k * TILE : (k + 1) * TILE] = 0.5 * f32(erow[k])
    for k in range(ecol.shape[0]):
        ec[k * TILE : (k + 1) * TILE] = 0.5 * f32(ecol[k])
    for q, shift in enumerate(shifts):
        xr[q] = er[pl.ds(TILE + shift, rows), :]
        xc[q] = b16(ec[pl.ds(TILE + shift, cols), :])
    steps = cols // TILE
    group = GROUP
    last = cols - 8
    middle = jnp.zeros((cols, LANES), jnp.float32)
    border = [jnp.zeros((cols, LANES), jnp.float32) for _ in range(3)]
    for chunk in range(rows // group):
        buf = lhs.at[chunk % lhs.shape[0]]
        for ii in range(group):
            i = chunk * group + ii
            edge_row = i < DMAX or i >= rows - DMAX
            row16 = [b16(jnp.broadcast_to(xr[q, i : i + 1, :], (TILE, LANES))) for q in range(6)]
            if edge_row:
                rmask = [b16(jnp.broadcast_to(mr[q, i : i + 1, :], (TILE, LANES))) for q in range(6)]
            for n in range(18):
                a, b = TAPS[n % 9]
                p, q = (a, 3 + b) if n < 9 else (3 + b, a)
                for s in range(steps):
                    value = row16[p] + xc[q, s * TILE : (s + 1) * TILE, :]
                    if s in (0, steps - 1):
                        value = value * mc[q, s * TILE : (s + 1) * TILE, :]
                    if edge_row:
                        value = value * rmask[p]
                    at = ii * cols + s * TILE
                    buf[at : at + TILE, n * LANES : (n + 1) * LANES] = value
        conv = dot(buf[...], wconv[...], ((1,), (1,))) + bias_row[...]
        base = chunk * group * cols
        acts[base : base + group * cols] = b16(jnp.maximum(conv, 0.0))
        grad = jnp.where(conv > 0, f32(guide[base : base + group * cols]), 0.0)
        row_sums = [[], [], []]
        for ii in range(group):
            i = chunk * group + ii
            g = grad[ii * cols : (ii + 1) * cols]
            inner = g[8:16]
            for s in range(2, cols // 8 - 1):
                inner = inner + g[s * 8 : (s + 1) * 8]
            for t in range(3):
                first, final = g[0:8], g[last:cols]
                if t != 1:
                    first, final = first * sm[t // 2, 0:8], final * sm[t // 2, last:cols]
                row_sums[t].append(jnp.sum(inner + first + final, axis=0, keepdims=True))
            if i < DMAX or i >= rows - DMAX:
                for t in range(3):
                    mask = g if t == 1 else g * jnp.broadcast_to(mr[6 + t // 2, i : i + 1, :], g.shape)
                    border[t] = border[t] + mask
            else:
                middle = middle + g
        for t in range(3):
            for s in range(group // 8):
                sums[chunk * group + s * 8 : chunk * group + (s + 1) * 8, t * LANES : (t + 1) * LANES] = (
                    jnp.concatenate(row_sums[t][s * 8 : (s + 1) * 8], axis=0)
                )
    for t in range(3):
        sums[rows : rows + cols, t * LANES : (t + 1) * LANES] = pltpu.roll(middle + border[t], MIRROR, 1)


def kernel_part(sums, xr, xc, send, kernel_tiles):
    stacked = b16(sums[...])
    x = [jnp.concatenate([b16(xr[q]), xc[q]], axis=0) for q in range(6)]
    wide = dot(stacked, jnp.concatenate(x, axis=1), ((0,), (0,)))
    filters = 48
    pieces = []
    for a, b in TAPS:
        tap = (
            wide[b * LANES : b * LANES + filters, a * LANES : (a + 1) * LANES]
            + wide[a * LANES + MIRROR : a * LANES + MIRROR + filters, (3 + b) * LANES : (4 + b) * LANES]
        )
        pieces += [tap[s * TILE : (s + 1) * TILE] for s in range(filters // TILE)]
    zero = jnp.zeros((TILE, LANES), jnp.bfloat16)
    for k in range(2 * kernel_tiles):
        send[k % 2, k // 2] = b16(pieces[k]) if k < len(pieces) else zero


def embedding_part(dil, half, sums, wall, prow, pcol, send, kernel_tiles, rows, cols):
    shifts = shift_list(dil)
    emb = 0.5 * dot(b16(sums[...]), wall[...], ((1,), (0,)))
    for q in range(6):
        part = emb[:, q * LANES : (q + 1) * LANES]
        prow[q, 24 : 24 + rows] = part[0:rows]
        pcol[q, 24 : 24 + cols] = part[rows : rows + cols]
    row_grad = sum(prow[q, pl.ds(8 - shifts[q], rows + 2 * TILE), :] for q in range(6))
    col_grad = sum(pcol[q, pl.ds(8 - shifts[q], cols + 2 * TILE), :] for q in range(6))
    zero = jnp.zeros((TILE, LANES), jnp.bfloat16)
    for k in range(6):
        send[k // 3, kernel_tiles + k % 3] = b16(col_grad[k * TILE : (k + 1) * TILE])
        send[k // 3, kernel_tiles + 3 + k % 3] = zero
    for k in range(4):
        value = b16(row_grad[k * TILE : (k + 1) * TILE])

        @pl.when(half == 0)
        def _():
            send[k // 3, kernel_tiles + 3 + k % 3] = value

        @pl.when(half == 1)
        def _():
            send[(k + 2) // 3, kernel_tiles + 3 + (k + 2) % 3] = value


def mix_maps(acts, mix_rows, mixb, contact):
    maps, rows, cols = contact.shape
    mix16 = b16(mix_rows[...])
    step = 8
    for chunk in range(rows // step):
        act = acts[chunk * step * cols : (chunk + 1) * step * cols]
        mixed = 0.5 * dot(mix16, act, ((1,), (1,)))
        contact[:, chunk * step : (chunk + 1) * step, :] = jnp.stack(
            [mixed[0:maps, ii * cols : (ii + 1) * cols] + mixb[...] for ii in range(step)], axis=1
        )


def compute_scratch(rows, cols):
    return [
        pltpu.VMEM((LANES, 18 * LANES), jnp.bfloat16),
        pltpu.VMEM((3 * LANES, 6 * LANES), jnp.bfloat16),
        pltpu.VMEM((1, LANES), jnp.float32),
        pltpu.VMEM((8, LANES), jnp.float32),
        pltpu.VMEM((rows + 2 * TILE, LANES), jnp.float32),
        pltpu.VMEM((cols + 2 * TILE, LANES), jnp.float32),
        pltpu.VMEM((6, rows, LANES), jnp.float32),
        pltpu.VMEM((6, cols, LANES), jnp.bfloat16),
        pltpu.VMEM((8, rows, LANES), jnp.float32),
        pltpu.VMEM((6, cols, LANES), jnp.bfloat16),
        pltpu.VMEM((2, cols, LANES), jnp.float32),
        pltpu.VMEM((5, rows, cols), jnp.float32),
        pltpu.VMEM((2, GROUP * cols, 18 * LANES), jnp.bfloat16),
        pltpu.VMEM((rows * cols, LANES), jnp.bfloat16),
        pltpu.VMEM((rows * cols, LANES), jnp.bfloat16),
        pltpu.VMEM((rows + cols, 3 * LANES), jnp.float32),
        pltpu.VMEM((6, rows + 48, LANES), jnp.float32),
        pltpu.VMEM((6, cols + 48, LANES), jnp.float32),
    ]


class Place:
    def __init__(self, n_row, n_col):
        self.n_col = n_col
        self.n_z = n_row // 4
        self.row = lax.axis_index("row")
        self.col = lax.axis_index("col")
        self.half = lax.rem(self.row, 2)
        self.chip = self.row // 2
        self.z = lax.rem(self.chip, self.n_z)
        self.y = self.chip // self.n_z
        self.partner = self.row + 1 - 2 * self.half
        self.far = lax.rem(self.row + n_row // 2, n_row)

    def z_peer(self, z):
        return self.row + 2 * (z - self.z)

    def plane_row(self, y):
        return self.row + 2 * self.n_z * (y - self.y)

    def plane(self):
        return [(y, c) for y in range(2) for c in range(self.n_col)]

    def is_me(self, y, c):
        return (self.y == y) & (self.col == c)


def greet_all(place, barrier):
    n_col, n_z = place.n_col, place.n_z
    to = [(place.partner, place.col)]
    to += [(place.row, lax.rem(place.col + d, n_col)) for d in range(1, n_col)]
    to += [(place.z_peer(lax.rem(place.z + d, n_z)), place.col) for d in range(1, n_z)]
    to += [(place.far, lax.rem(place.col + d, n_col)) for d in range(n_col)]
    to += [(place.partner, lax.rem(place.col + d, n_col)) for d in (1, n_col - 1)]
    for device in to:
        pl.semaphore_signal(barrier, inc=1, device_id=device, device_id_type=MESH)
    return len(to)


def remote(src, dst, send_sem, recv_sem, row, col):
    return pltpu.make_async_remote_copy(
        src_ref=src, dst_ref=dst, send_sem=send_sem, recv_sem=recv_sem, device_id=(row, col), device_id_type=MESH
    )


def total(ref, count):
    value = f32(ref[0])
    for k in range(1, count):
        value = value + f32(ref[k])
    return value


class Exchange:
    def __init__(self, place, emb, erow, ecol, main_s, side_s, edge_s, recv_s):
        self.p, self.emb, self.erow, self.ecol = place, emb, erow, ecol
        self.main_s, self.side_s, self.edge_s, self.recv_s = main_s, side_s, edge_s, recv_s
        half = place.half
        self.side = place.chip - 1 + 2 * half
        self.side_ok = (self.side >= 0) & (self.side < place.n_col)
        self.low_ok = place.col > 0
        self.high_ok = place.col < place.n_col - 1

    def main(self, dst):
        h = self.p.half
        return remote(
            self.emb.at[pl.ds(h, 3)], self.erow.at[pl.ds(1 - h, 3)],
            self.main_s.at[dst], self.recv_s.at[0], self.p.row, dst,
        )

    def margin(self, dst):
        h = self.p.half
        return remote(
            self.emb.at[3 - 3 * h], self.erow.at[3 * h],
            self.side_s.at[dst], self.recv_s.at[1], self.p.row, dst,
        )

    def up(self, dst):
        return remote(self.emb.at[3], self.ecol.at[0], self.edge_s.at[0], self.recv_s.at[2], self.p.row, dst)

    def down(self, dst):
        return remote(self.emb.at[0], self.ecol.at[5], self.edge_s.at[1], self.recv_s.at[3], self.p.row, dst)

    def start(self):
        p = self.p
        for k, (owner, copy) in enumerate(((p.chip, self.main), (self.side, self.margin))):

            @pl.when(p.col == owner)
            def _():
                for dst in range(p.n_col):

                    @pl.when(p.col != dst)
                    def _():
                        copy(dst).start()

        @pl.when(self.high_ok)
        def _():
            self.up(p.col + 1).start()

        @pl.when(self.low_ok)
        def _():
            self.down(p.col - 1).start()

    def local(self):
        p = self.p
        for k in range(4):
            self.ecol[1 + k] = self.emb[k]

        @pl.when(p.col == p.chip)
        def _():
            for k in range(3):
                self.erow[1 - p.half + k] = self.emb[p.half + k]

        @pl.when(p.col == self.side)
        def _():
            self.erow[3 * p.half] = self.emb[3 - 3 * p.half]

        zero = jnp.zeros(self.emb.shape[1:], self.emb.dtype)

        @pl.when(jnp.logical_not(self.side_ok))
        def _():
            self.erow[3 * p.half] = zero

        @pl.when(jnp.logical_not(self.low_ok))
        def _():
            self.ecol[0] = zero

        @pl.when(jnp.logical_not(self.high_ok))
        def _():
            self.ecol[5] = zero

    def finish(self):
        p = self.p

        @pl.when(p.col != p.chip)
        def _():
            self.main(p.col).wait_recv()

        @pl.when((p.col != self.side) & self.side_ok)
        def _():
            self.margin(p.col).wait_recv()

        @pl.when(self.low_ok)
        def _():
            self.up(p.col).wait_recv()

        @pl.when(self.high_ok)
        def _():
            self.down(p.col).wait_recv()

    def sent(self):
        p = self.p
        for owner, copy in ((p.chip, self.main), (self.side, self.margin)):

            @pl.when(p.col == owner)
            def _():
                for dst in range(p.n_col):

                    @pl.when(p.col != dst)
                    def _():
                        copy(dst).wait_send()

        @pl.when(self.high_ok)
        def _():
            self.up(p.col).wait_send()

        @pl.when(self.low_ok)
        def _():
            self.down(p.col).wait_send()


def fused_kernel(
    n_row, n_col, owners, per_owner, rows, cols, bins,
    dil, emb, kern, bias, mix, mixb, cot,
    contact, kernel_out, emb_out,
    *scratch,
):
    place = Place(n_row, n_col)
    n_z = place.n_z
    row, col, half = place.row, place.col, place.half
    kt = per_owner * owners
    n_compute = 18
    (wconv, wall, bias_row, mix_rows, er, ec, xr, xc, mr, mc, sm, cotf, lhs, guide, acts, sums, prow, pcol) = scratch[
        :n_compute
    ]
    (
        erow, ecol, send, core_in, own, r_kernel, r_row, p_emb, y_emb, z_kernel, z_emb, full, emb_all, margins,
        main_s, side_s, edge_s, recv_s, core_s, kern_s, row_s, y_s, zk_s, ze_s, ag_s, agc_s, fin_s,
    ) = scratch[n_compute:]

    margins[...] = jnp.zeros_like(margins)
    barrier = pltpu.get_barrier_semaphore()
    count = greet_all(place, barrier)
    load_weights(kern, bias, mix, wconv, wall, bias_row, mix_rows)
    pl.semaphore_wait(barrier, count)

    exchange = Exchange(place, emb, erow, ecol, main_s, side_s, edge_s, recv_s)
    exchange.start()
    exchange.local()
    prow[...] = jnp.zeros_like(prow)
    pcol[...] = jnp.zeros_like(pcol)
    prepare(dil, place, cot, mr, mc, sm, cotf, mix_rows, guide, rows, cols, bins)
    exchange.finish()

    convolve(dil, erow, ecol, wconv, bias_row, er, ec, xr, xc, mr, mc, sm, lhs, guide, acts, sums, rows, cols)

    kernel_part(sums, xr, xc, send, kt)

    def swap(n, at, size):
        return remote(
            send.at[1 - half, pl.ds(at, size)], core_in.at[pl.ds(at, size)],
            core_s.at[0, n], core_s.at[1, n], place.partner, col,
        )

    swap(0, 0, kt).start()
    embedding_part(dil, half, sums, wall, prow, pcol, send, kt, rows, cols)
    swap(1, kt, 6).start()

    def owner_of(n):
        return place.plane_row(n % 2), n

    owner = (col < owners) & (lax.rem(col, 2) == place.y)

    def kernel_copy(slot, n):
        to_row, to_col = owner_of(n)
        return remote(
            own.at[pl.ds(n * per_owner, per_owner)], r_kernel.at[slot],
            kern_s.at[0, n], kern_s.at[1, slot], to_row, to_col,
        )

    my_slot = place.y * n_col + col
    swap(0, 0, kt).wait()
    own[0:kt] = b16(f32(send[half, 0:kt]) + f32(core_in[0:kt]))
    for n in range(owners):

        @pl.when(jnp.logical_not(place.is_me(n % 2, n)))
        def _():
            kernel_copy(my_slot, n).start()

    def row_copy(src):
        return remote(own.at[pl.ds(kt + 3, 3)], r_row.at[src], row_s.at[n_col], row_s.at[src], row, place.chip)

    swap(1, kt, 6).wait()
    own[kt : kt + 6] = b16(f32(send[half, kt : kt + 6]) + f32(core_in[kt : kt + 6]))

    @pl.when(col != place.chip)
    def _():
        row_copy(col).start()

    @pl.when(owner)
    def _():
        r_kernel[my_slot] = own[pl.ds(col * per_owner, per_owner)]

    @pl.when(col == place.chip)
    def _():
        r_row[col] = own[kt + 3 : kt + 6]

    mix_maps(acts, mix_rows, mixb, contact)

    far_copy = remote(p_emb, y_emb, y_s.at[0], y_s.at[1], place.far, col)

    def z_copy(sems, buf, src, dst):
        return remote(buf.at[src], buf.at[src], sems.at[0, dst], sems.at[1, src], place.z_peer(dst), col)

    def kernel_in(slot):
        return remote(
            own.at[pl.ds(0, per_owner)], r_kernel.at[slot], kern_s.at[0, 0], kern_s.at[1, slot], row, col
        )

    @pl.when(owner)
    def _():
        for slot, (y, c) in enumerate(place.plane()):

            @pl.when(jnp.logical_not(place.is_me(y, c)))
            def _():
                kernel_in(slot).wait_recv()

        z_kernel[place.z] = b16(total(r_kernel, 2 * n_col))
        for dst in range(n_z):

            @pl.when(dst != place.z)
            def _():
                z_copy(zk_s, z_kernel, place.z, dst).start()

    mine = f32(own[kt : kt + 3])

    @pl.when(col != place.chip)
    def _():
        p_emb[...] = b16(mine)

    @pl.when(col == place.chip)
    def _():
        for src in range(n_col):

            @pl.when(src != col)
            def _():
                row_copy(src).wait_recv()

        p_emb[...] = b16(mine + total(r_row, n_col))

    far_copy.start()

    def gather_copy(n, y, c):
        return remote(full.at[half, n], full.at[half, n], ag_s.at[0, y * n_col + c], ag_s.at[1, n], place.plane_row(y), c)

    @pl.when(owner)
    def _():
        for src in range(n_z):

            @pl.when(src != place.z)
            def _():
                z_copy(zk_s, z_kernel, src, place.z).wait_recv()

        full[half, col] = b16(total(z_kernel, n_z))
        for y, c in place.plane():

            @pl.when(jnp.logical_not(place.is_me(y, c)))
            def _():
                gather_copy(col, y, c).start()

    far_copy.wait()
    z_emb[place.z] = b16(f32(p_emb[...]) + f32(y_emb[...]))
    for dst in range(n_z):

        @pl.when(dst != place.z)
        def _():
            z_copy(ze_s, z_emb, place.z, dst).start()

    for src in range(n_z):

        @pl.when(src != place.z)
        def _():
            z_copy(ze_s, z_emb, src, place.z).wait_recv()

    emb_all[half] = b16(total(z_emb, n_z))
    emb_swap = remote(emb_all.at[half], emb_all.at[half], fin_s.at[0, 0], fin_s.at[1, 0], place.partner, col)
    emb_swap.start()
    to = col - 1 + 2 * half
    exists = (to >= 0) & (to < n_col)
    came = col + 1 - 2 * half
    came_ok = (came >= 0) & (came < n_col)

    def margin_copy(n, slot, device_row, device_col):
        return remote(
            emb_all.at[half, 2 * half], margins.at[slot],
            fin_s.at[0, 1 + n], fin_s.at[1, 1 + n], device_row, device_col,
        )

    @pl.when(exists)
    def _():
        margin_copy(0, half, row, to).start()
        margin_copy(1, half, place.partner, to).start()

    for n in range(owners):

        @pl.when(jnp.logical_not(place.is_me(n % 2, n)))
        def _():
            gather_copy(n, place.y, col).wait_recv()

    share = remote(full.at[half], full.at[half], agc_s.at[0], agc_s.at[1], place.partner, col)
    share.start()

    emb_swap.wait()

    @pl.when(came_ok)
    def _():
        margin_copy(0, half, row, col).wait_recv()

    @pl.when(exists)
    def _():
        margin_copy(1, 1 - half, row, col).wait_recv()

    main = [f32(emb_all[0, 1]), f32(emb_all[0, 2]), f32(emb_all[1, 0]), f32(emb_all[1, 1])]
    emb_out[0] = main[0] + f32(margins[1])
    emb_out[1] = main[1]
    emb_out[2] = main[2]
    emb_out[3] = main[3] + f32(margins[0])

    exchange.sent()
    for n in range(owners):

        @pl.when(jnp.logical_not(place.is_me(n % 2, n)))
        def _():
            kernel_copy(my_slot, n).wait_send()

    @pl.when(col != place.chip)
    def _():
        row_copy(col).wait_send()

    for dst in range(n_z):

        @pl.when((dst != place.z) & owner)
        def _():
            z_copy(zk_s, z_kernel, place.z, dst).wait_send()

        @pl.when(dst != place.z)
        def _():
            z_copy(ze_s, z_emb, place.z, dst).wait_send()

    @pl.when(owner)
    def _():
        for y, c in place.plane():

            @pl.when(jnp.logical_not(place.is_me(y, c)))
            def _():
                gather_copy(col, y, c).wait_send()

    @pl.when(exists)
    def _():
        margin_copy(0, half, row, to).wait_send()
        margin_copy(1, half, place.partner, to).wait_send()

    share.wait()
    kernel_out[...] = full[...]


def fused_scratch(n_row, n_col, owners, per_owner):
    n_z = n_row // 4
    kt = owners * per_owner

    def tiles(*lead):
        return pltpu.VMEM((*lead, TILE, LANES), jnp.bfloat16)

    def sems(*shape):
        return pltpu.SemaphoreType.DMA(shape)

    return [
        tiles(4), tiles(6), tiles(2, kt + 6), tiles(kt + 6), tiles(kt + 6), tiles(2 * n_col, per_owner), tiles(n_col, 3),
        tiles(3), tiles(3), tiles(n_z, per_owner), tiles(n_z, 3), tiles(2, owners, per_owner), tiles(2, 3), tiles(2),
        sems(n_col), sems(n_col), sems(2), sems(4), sems(2, 2), sems(2, 2 * n_col), sems(n_col + 1), sems(2),
        sems(2, n_z), sems(2, n_z), sems(2, 2 * n_col), sems(2), sems(2, 3),
    ]


def finish_kernel(per_owner, contact, grad, emb, contact_out, grad_out, emb_out):
    contact_out[...] = contact[...]
    emb_out[...] = emb[...]
    for k in range(grad_out.shape[0]):
        grad_out[k] = f32(grad[k % 2, k // (2 * per_owner), (k // 2) % per_owner])


def per_device(n_row, n_col, embedding, dilation, kernel, kernel_bias, mixing, mixing_bias, cotangent):
    channels = embedding.shape[1]
    filters = kernel.shape[2]
    maps, rows, cols = cotangent.shape
    bins = cols * n_col
    count = 9 * filters // TILE
    per_owner = -(-count // (2 * n_col))
    owners = -(-count // (2 * per_owner))
    contact, grad, emb = pl.pallas_call(
        functools.partial(fused_kernel, n_row, n_col, owners, per_owner, rows, cols, bins),
        out_shape=[
            jax.ShapeDtypeStruct((maps, rows, cols), jnp.float32),
            jax.ShapeDtypeStruct((2, owners, per_owner, TILE, channels), jnp.bfloat16),
            jax.ShapeDtypeStruct((cols // TILE, TILE, channels), jnp.float32),
        ],
        in_specs=[SM, VM, VM, VM, VM, VM, VM],
        out_specs=[VM, VM, VM],
        scratch_shapes=compute_scratch(rows, cols) + fused_scratch(n_row, n_col, owners, per_owner),
        compiler_params=pltpu.CompilerParams(collective_id=0, has_side_effects=True),
    )(
        dilation,
        embedding.reshape(cols // TILE, TILE, channels),
        kernel,
        kernel_bias[None],
        mixing,
        mixing_bias[:, None],
        cotangent,
    )
    contact, grad, emb = pl.pallas_call(
        functools.partial(finish_kernel, per_owner),
        out_shape=[
            jax.ShapeDtypeStruct((maps, rows, cols), jnp.float32),
            jax.ShapeDtypeStruct((count, TILE, channels), jnp.float32),
            jax.ShapeDtypeStruct((cols // TILE, TILE, channels), jnp.float32),
        ],
        in_specs=[VM, VM, VM],
        out_specs=[VM, VM, VM],
    )(contact, grad, emb)
    return contact, emb.reshape(cols, channels), grad.reshape(3, 3, filters, channels)


def solution(mesh):
    return jax.shard_map(
        functools.partial(per_device, mesh.shape["row"], mesh.shape["col"]),
        mesh=mesh,
        in_specs=(P("col", None), P(), P(), P(), P(), P(), P(None, "row", "col")),
        out_specs=(P(None, "row", "col"), P("col", None), P()),
        check_vma=False,
    )
```

```python
import functools

import jax
import jax.numpy as jnp
from jax import lax
from jax.experimental import pallas as pl
from jax.experimental.pallas import tpu as pltpu
from jax.sharding import PartitionSpec as P

MESH = pl.DeviceIdType.MESH
DMAX = 4
TILE = 16
LANES = 128
MIRROR = 64
GROUP = 8
N_LO = 4
VMEM = 20 << 20
NEAR = (-1, 0, 1, 2)
TAPS = [(a, b) for a in range(3) for b in range(3)]
VM = pl.BlockSpec(memory_space=pltpu.VMEM)
SM = pl.BlockSpec(memory_space=pltpu.SMEM)


def f32(value):
    return value.astype(jnp.float32)


def b16(value):
    return value.astype(jnp.bfloat16)


def dot(a, b, dims):
    return lax.dot_general(a, b, (dims, ((), ())), preferred_element_type=jnp.float32)


def load_weights(kern, bias, mix, wconv, wall, bias_row, mix_rows):
    filters = kern.shape[2]
    wconv[...] = jnp.zeros_like(wconv)
    wall[...] = jnp.zeros_like(wall)
    bias_row[...] = jnp.zeros_like(bias_row)
    mix_rows[...] = jnp.zeros_like(mix_rows)
    for at in (0, MIRROR):
        bias_row[:, at : at + filters] = bias[...]
        mix_rows[0 : mix.shape[0], at : at + filters] = f32(mix[...])
    for n, (a, b) in enumerate(TAPS):
        tap = kern[a, b]
        wconv[0:filters, n * LANES : (n + 1) * LANES] = tap
        wconv[MIRROR : MIRROR + filters, (9 + n) * LANES : (10 + n) * LANES] = tap
        wall[b * LANES : b * LANES + filters, a * LANES : (a + 1) * LANES] = tap
        wall[a * LANES + MIRROR : a * LANES + MIRROR + filters, (3 + b) * LANES : (4 + b) * LANES] = tap


def shift_list(dil):
    return [-dil[0], 0, dil[0], -dil[1], 0, dil[1]]


def prepare(dil, place, cot, mr, mc, sm, cotf, mix_rows, guide, rows, cols, bins):
    row_rate, col_rate = dil[0], dil[1]
    lane_r = lax.broadcasted_iota(jnp.int32, (rows, LANES), 1)
    lane_c = lax.broadcasted_iota(jnp.int32, (cols, LANES), 1)
    row_at = lax.broadcasted_iota(jnp.int32, (rows, LANES), 0) + place.row * rows
    col_at = lax.broadcasted_iota(jnp.int32, (cols, LANES), 0) + place.col * cols

    def inside(at):
        return jnp.where((at >= 0) & (at < bins), 1.0, 0.0)

    for q, shift in enumerate(shift_list(dil)):
        mr[q] = inside(row_at + shift)
        mc[q] = b16(inside(col_at + shift))
    for n, t in enumerate((-1, 1)):
        mr[6 + n] = inside(row_at + jnp.where(lane_r < MIRROR, t * row_rate, t * col_rate))
        sm[n] = inside(col_at + jnp.where(lane_c < MIRROR, t * col_rate, t * row_rate))
    cotf[...] = f32(cot[...])
    mix16 = b16(mix_rows[...])
    for i in range(rows):
        guide[i * cols : (i + 1) * cols] = b16(0.5 * dot(b16(cotf[:, i, :]), mix16[0 : cotf.shape[0]], ((0,), (0,))))


def convolve(dil, erow, ecol, wconv, bias_row, er, ec, xr, xc, mr, mc, sm, lhs, guide, acts, sums, rows, cols):
    shifts = shift_list(dil)
    for k in range(erow.shape[0]):
        er[k * TILE : (k + 1) * TILE] = 0.5 * f32(erow[k])
    for k in range(ecol.shape[0]):
        ec[k * TILE : (k + 1) * TILE] = 0.5 * f32(ecol[k])
    for q, shift in enumerate(shifts):
        xr[q] = er[pl.ds(TILE + shift, rows), :]
        xc[q] = b16(ec[pl.ds(TILE + shift, cols), :])
    steps = cols // TILE
    group = GROUP
    last = cols - 8
    middle = jnp.zeros((cols, LANES), jnp.float32)
    border = [jnp.zeros((cols, LANES), jnp.float32) for _ in range(3)]
    for chunk in range(rows // group):
        buf = lhs.at[chunk % lhs.shape[0]]
        for ii in range(group):
            i = chunk * group + ii
            edge_row = i < DMAX or i >= rows - DMAX
            row16 = [b16(jnp.broadcast_to(xr[q, i : i + 1, :], (TILE, LANES))) for q in range(6)]
            if edge_row:
                rmask = [b16(jnp.broadcast_to(mr[q, i : i + 1, :], (TILE, LANES))) for q in range(6)]
            for n in range(18):
                a, b = TAPS[n % 9]
                p, q = (a, 3 + b) if n < 9 else (3 + b, a)
                for s in range(steps):
                    value = row16[p] + xc[q, s * TILE : (s + 1) * TILE, :]
                    if s in (0, steps - 1):
                        value = value * mc[q, s * TILE : (s + 1) * TILE, :]
                    if edge_row:
                        value = value * rmask[p]
                    at = ii * cols + s * TILE
                    buf[at : at + TILE, n * LANES : (n + 1) * LANES] = value
        conv = dot(buf[...], wconv[...], ((1,), (1,))) + bias_row[...]
        base = chunk * group * cols
        acts[base : base + group * cols] = b16(jnp.maximum(conv, 0.0))
        grad = jnp.where(conv > 0, f32(guide[base : base + group * cols]), 0.0)
        row_sums = [[], [], []]
        for ii in range(group):
            i = chunk * group + ii
            g = grad[ii * cols : (ii + 1) * cols]
            inner = g[8:16]
            for s in range(2, cols // 8 - 1):
                inner = inner + g[s * 8 : (s + 1) * 8]
            for t in range(3):
                first, final = g[0:8], g[last:cols]
                if t != 1:
                    first, final = first * sm[t // 2, 0:8], final * sm[t // 2, last:cols]
                row_sums[t].append(jnp.sum(inner + first + final, axis=0, keepdims=True))
            if i < DMAX or i >= rows - DMAX:
                for t in range(3):
                    mask = g if t == 1 else g * jnp.broadcast_to(mr[6 + t // 2, i : i + 1, :], g.shape)
                    border[t] = border[t] + mask
            else:
                middle = middle + g
        for t in range(3):
            for s in range(group // 8):
                sums[chunk * group + s * 8 : chunk * group + (s + 1) * 8, t * LANES : (t + 1) * LANES] = (
                    jnp.concatenate(row_sums[t][s * 8 : (s + 1) * 8], axis=0)
                )
    for t in range(3):
        sums[rows : rows + cols, t * LANES : (t + 1) * LANES] = pltpu.roll(middle + border[t], MIRROR, 1)


def kernel_part(sums, xr, xc, send, kernel_tiles):
    stacked = b16(sums[...])
    x = [jnp.concatenate([b16(xr[q]), xc[q]], axis=0) for q in range(6)]
    wide = dot(stacked, jnp.concatenate(x, axis=1), ((0,), (0,)))
    filters = 48
    pieces = []
    for a, b in TAPS:
        tap = (
            wide[b * LANES : b * LANES + filters, a * LANES : (a + 1) * LANES]
            + wide[a * LANES + MIRROR : a * LANES + MIRROR + filters, (3 + b) * LANES : (4 + b) * LANES]
        )
        pieces += [tap[s * TILE : (s + 1) * TILE] for s in range(filters // TILE)]
    zero = jnp.zeros((TILE, LANES), jnp.bfloat16)
    for k in range(2 * kernel_tiles):
        send[k % 2, k // 2] = b16(pieces[k]) if k < len(pieces) else zero


def embedding_part(dil, half, sums, wall, prow, pcol, send, kernel_tiles, rows, cols):
    shifts = shift_list(dil)
    emb = 0.5 * dot(b16(sums[...]), wall[...], ((1,), (0,)))
    for q in range(6):
        part = emb[:, q * LANES : (q + 1) * LANES]
        prow[q, 24 : 24 + rows] = part[0:rows]
        pcol[q, 24 : 24 + cols] = part[rows : rows + cols]
    row_grad = sum(prow[q, pl.ds(8 - shifts[q], rows + 2 * TILE), :] for q in range(6))
    col_grad = sum(pcol[q, pl.ds(8 - shifts[q], cols + 2 * TILE), :] for q in range(6))
    zero = jnp.zeros((TILE, LANES), jnp.bfloat16)
    for k in range(6):
        send[k // 3, kernel_tiles + k % 3] = b16(col_grad[k * TILE : (k + 1) * TILE])
        send[k // 3, kernel_tiles + 3 + k % 3] = zero
    for k in range(4):
        value = b16(row_grad[k * TILE : (k + 1) * TILE])

        @pl.when(half == 0)
        def _():
            send[k // 3, kernel_tiles + 3 + k % 3] = value

        @pl.when(half == 1)
        def _():
            send[(k + 2) // 3, kernel_tiles + 3 + (k + 2) % 3] = value


def mix_maps(acts, mix_rows, mixb, contact):
    maps, rows, cols = contact.shape
    mix16 = b16(mix_rows[...])
    step = 8
    at = lax.broadcasted_iota(jnp.int32, (8, step * cols), 0)
    offset = jnp.zeros((8, step * cols), jnp.float32)
    for t in range(maps):
        offset = jnp.where(at == t, mixb[t], offset)
    for chunk in range(rows // step):
        act = acts[chunk * step * cols : (chunk + 1) * step * cols]
        mixed = 0.5 * dot(mix16, act, ((1,), (1,))) + offset
        contact[:, chunk * step : (chunk + 1) * step, :] = jnp.stack(
            [mixed[0:maps, ii * cols : (ii + 1) * cols] for ii in range(step)], axis=1
        )


def compute_scratch(rows, cols):
    return [
        pltpu.VMEM((LANES, 18 * LANES), jnp.bfloat16),
        pltpu.VMEM((3 * LANES, 6 * LANES), jnp.bfloat16),
        pltpu.VMEM((1, LANES), jnp.float32),
        pltpu.VMEM((8, LANES), jnp.float32),
        pltpu.VMEM((rows + 2 * TILE, LANES), jnp.float32),
        pltpu.VMEM((cols + 2 * TILE, LANES), jnp.float32),
        pltpu.VMEM((6, rows, LANES), jnp.float32),
        pltpu.VMEM((6, cols, LANES), jnp.bfloat16),
        pltpu.VMEM((8, rows, LANES), jnp.float32),
        pltpu.VMEM((6, cols, LANES), jnp.bfloat16),
        pltpu.VMEM((2, cols, LANES), jnp.float32),
        pltpu.VMEM((5, rows, cols), jnp.float32),
        pltpu.VMEM((2, GROUP * cols, 18 * LANES), jnp.bfloat16),
        pltpu.VMEM((rows * cols, LANES), jnp.bfloat16),
        pltpu.VMEM((rows * cols, LANES), jnp.bfloat16),
        pltpu.VMEM((rows + cols, 3 * LANES), jnp.float32),
        pltpu.VMEM((6, rows + 48, LANES), jnp.float32),
        pltpu.VMEM((6, cols + 48, LANES), jnp.float32),
    ]


class Place:
    def __init__(self, n_row, n_col):
        self.n_col = n_col
        self.n_z = n_row // 4
        self.row = lax.axis_index("row")
        self.col = lax.axis_index("col")
        self.half = lax.rem(self.row, 2)
        self.chip = self.row // 2
        self.z = lax.rem(self.chip, self.n_z)
        self.y = self.chip // self.n_z
        self.n_lo = N_LO
        self.n_x = n_col // N_LO
        self.n_y = 2 * N_LO
        self.x = self.col // N_LO
        self.yy = self.y * N_LO + lax.rem(self.col, N_LO)
        self.partner = self.row + 1 - 2 * self.half
        self.far = lax.rem(self.row + n_row // 2, n_row)

    def z_peer(self, z):
        return self.row + 2 * (z - self.z)

    def plane_row(self, y):
        return self.row + 2 * self.n_z * (y - self.y)

    def turn(self, step):
        return lax.rem(self.yy + step + self.n_y, self.n_y)

    def at(self, x, yy):
        return self.plane_row(yy // self.n_lo), x * self.n_lo + lax.rem(yy, self.n_lo)

    def plane(self):
        return [(y, c) for y in range(2) for c in range(self.n_col)]

    def is_me(self, y, c):
        return (self.y == y) & (self.col == c)


def greet_all(place, barrier):
    n_col, n_z = place.n_col, place.n_z
    to = [(place.partner, place.col)]
    to += [
        place.at(lax.rem(place.x + dx, place.n_x), place.turn(dy))
        for dx in range(place.n_x)
        for dy in (-2, -1, 0, 1, 2)
        if dx or dy
    ]
    to += [(place.z_peer(lax.rem(place.z + d, n_z)), place.col) for d in range(1, n_z)]
    to += [(place.partner, lax.rem(place.col + d, n_col)) for d in (1, n_col - 1)]
    for device in to:
        pl.semaphore_signal(barrier, inc=1, device_id=device, device_id_type=MESH)
    return len(to)


def greet_far(place, second):
    for dy in (-2, 2):
        pl.semaphore_signal(second, inc=1, device_id=place.at(place.x, place.turn(dy)), device_id_type=MESH)


def remote(src, dst, send_sem, recv_sem, row, col):
    return pltpu.make_async_remote_copy(
        src_ref=src, dst_ref=dst, send_sem=send_sem, recv_sem=recv_sem, device_id=(row, col), device_id_type=MESH
    )


def total(ref, count):
    value = f32(ref[0])
    for k in range(1, count):
        value = value + f32(ref[k])
    return value


class Exchange:
    def __init__(self, place, emb, erow, ecol, main_s, side_s, edge_s, recv_s):
        self.p, self.emb, self.erow, self.ecol = place, emb, erow, ecol
        self.main_s, self.side_s, self.edge_s, self.recv_s = main_s, side_s, edge_s, recv_s
        half, col, z = place.half, place.col, place.z
        self.side = place.chip - 1 + 2 * half
        self.side_ok = (self.side >= 0) & (self.side < place.n_col)
        self.low_ok = col > 0
        self.high_ok = col < place.n_col - 1
        self.main_src = (col == z) | (col == place.n_z + z)
        self.main_y = jnp.where(col == z, 0, 1)
        side = z - 1 + 2 * half
        self.side_src = (col == side) | (col == place.n_z + side)
        self.side_y = jnp.where(col == side, 0, 1)

    def targets(self, for_y):
        p = self.p
        for k, dy in enumerate(NEAR):
            yy = p.turn(dy)
            for x in range(p.n_x):
                wanted = yy // p.n_lo == for_y
                if dy == 0:
                    wanted = wanted & (x != p.x)
                yield k * p.n_x + x, wanted, *p.at(x, yy)

    def main(self, slot, row, col):
        h = self.p.half
        return remote(
            self.emb.at[pl.ds(h, 3)], self.erow.at[pl.ds(1 - h, 3)],
            self.main_s.at[slot], self.recv_s.at[0], row, col,
        )

    def margin(self, slot, row, col):
        h = self.p.half
        return remote(
            self.emb.at[3 - 3 * h], self.erow.at[3 * h],
            self.side_s.at[slot], self.recv_s.at[1], row, col,
        )

    def up(self):
        p = self.p
        row = p.plane_row(p.turn(1) // p.n_lo)
        return remote(self.emb.at[3], self.ecol.at[0], self.edge_s.at[0], self.recv_s.at[2], row, p.col + 1)

    def down(self):
        p = self.p
        row = p.plane_row(p.turn(-1) // p.n_lo)
        return remote(self.emb.at[0], self.ecol.at[5], self.edge_s.at[1], self.recv_s.at[3], row, p.col - 1)

    def outgoing(self, act):
        for source, for_y, copy in (
            (self.main_src, self.main_y, self.main),
            (self.side_src, self.side_y, self.margin),
        ):

            @pl.when(source)
            def _():
                for slot, wanted, row, col in self.targets(for_y):

                    @pl.when(wanted)
                    def _():
                        act(copy(slot, row, col))

        @pl.when(self.high_ok)
        def _():
            act(self.up())

        @pl.when(self.low_ok)
        def _():
            act(self.down())

    def start(self):
        self.outgoing(lambda copy: copy.start())

    def sent(self):
        self.outgoing(lambda copy: copy.wait_send())

    def local(self):
        p = self.p
        for k in range(4):
            self.ecol[1 + k] = self.emb[k]

        @pl.when(p.col == p.chip)
        def _():
            for k in range(3):
                self.erow[1 - p.half + k] = self.emb[p.half + k]

        @pl.when(p.col == self.side)
        def _():
            self.erow[3 * p.half] = self.emb[3 - 3 * p.half]

        zero = jnp.zeros(self.emb.shape[1:], self.emb.dtype)

        @pl.when(jnp.logical_not(self.side_ok))
        def _():
            self.erow[3 * p.half] = zero

        @pl.when(jnp.logical_not(self.low_ok))
        def _():
            self.ecol[0] = zero

        @pl.when(jnp.logical_not(self.high_ok))
        def _():
            self.ecol[5] = zero

    def finish(self):
        p = self.p

        @pl.when(p.col != p.chip)
        def _():
            self.main(0, p.row, p.col).wait_recv()

        @pl.when((p.col != self.side) & self.side_ok)
        def _():
            self.margin(0, p.row, p.col).wait_recv()

        @pl.when(self.low_ok)
        def _():
            self.up().wait_recv()

        @pl.when(self.high_ok)
        def _():
            self.down().wait_recv()


def fused_kernel(
    n_row, n_col, owners, per_owner, rows, cols, bins,
    dil_h, emb_h, kern_h, bias_h, mix_h, mixb_h, cot_h,
    contact, kernel_out, emb_out,
    *scratch,
):
    place = Place(n_row, n_col)
    n_z = place.n_z
    row, col, half = place.row, place.col, place.half
    kt = per_owner * owners
    n_compute = 18
    (wconv, wall, bias_row, mix_rows, er, ec, xr, xc, mr, mc, sm, cotf, lhs, guide, acts, sums, prow, pcol) = scratch[
        :n_compute
    ]
    (
        erow, ecol, send, core_in, own, r_kernel, r_row, p_emb, y_emb, z_kernel, z_emb, full, emb_all, margins,
        main_s, side_s, edge_s, recv_s, core_s, kern_s, row_s, y_s, zk_s, ze_s, ag_s, agc_s, fin_s,
        second, emb, dil, kern, bias, mix, mixb, cot, load_s,
    ) = scratch[n_compute:]

    margins[...] = jnp.zeros_like(margins)
    r_row[...] = jnp.zeros_like(r_row)
    barrier = pltpu.get_barrier_semaphore()
    count = greet_all(place, barrier)
    loads = [
        pltpu.make_async_copy(src, dst, load_s.at[n])
        for n, (src, dst) in enumerate(
            ((emb_h, emb), (dil_h, dil), (kern_h, kern), (bias_h, bias), (mix_h, mix), (mixb_h, mixb), (cot_h, cot))
        )
    ]
    for load in loads:
        load.start()
    prow[...] = jnp.zeros_like(prow)
    pcol[...] = jnp.zeros_like(pcol)
    for load in loads:
        load.wait()
    load_weights(kern, bias, mix, wconv, wall, bias_row, mix_rows)
    exchange = Exchange(place, emb, erow, ecol, main_s, side_s, edge_s, recv_s)
    exchange.local()
    pl.semaphore_wait(barrier, count)

    exchange.start()
    greet_far(place, second)
    prepare(dil, place, cot, mr, mc, sm, cotf, mix_rows, guide, rows, cols, bins)
    exchange.finish()

    convolve(dil, erow, ecol, wconv, bias_row, er, ec, xr, xc, mr, mc, sm, lhs, guide, acts, sums, rows, cols)

    kernel_part(sums, xr, xc, send, kt)

    def swap(n, at, size):
        return remote(
            send.at[1 - half, pl.ds(at, size)], core_in.at[pl.ds(at, size)],
            core_s.at[0, n], core_s.at[1, n], place.partner, col,
        )

    swap(0, 0, kt).start()
    embedding_part(dil, half, sums, wall, prow, pcol, send, kt, rows, cols)
    swap(1, kt, 6).start()

    def owner_of(n):
        return place.plane_row(n % 2), n

    owner = (col < owners) & (lax.rem(col, 2) == place.y)

    def kernel_copy(slot, n):
        to_row, to_col = owner_of(n)
        return remote(
            own.at[pl.ds(n * per_owner, per_owner)], r_kernel.at[slot],
            kern_s.at[0, n], kern_s.at[1, slot], to_row, to_col,
        )

    my_slot = place.y * n_col + col
    pl.semaphore_wait(second, 2)
    swap(0, 0, kt).wait()
    own[0:kt] = b16(f32(send[half, 0:kt]) + f32(core_in[0:kt]))
    for n in range(owners):

        @pl.when(jnp.logical_not(place.is_me(n % 2, n)))
        def _():
            kernel_copy(my_slot, n).start()

    ahead = lax.rem(place.yy - lax.rem(place.chip, N_LO) + 1 + place.n_y, place.n_y)
    row_slot = lax.rem(ahead, 4) * place.n_x + place.x
    row_to = place.plane_row(jnp.where(ahead < 4, 0, 1))

    def row_copy(slot):
        return remote(own.at[pl.ds(kt + 3, 3)], r_row.at[slot], row_s.at[0], row_s.at[1 + slot], row_to, place.chip)

    swap(1, kt, 6).wait()
    own[kt : kt + 6] = b16(f32(send[half, kt : kt + 6]) + f32(core_in[kt : kt + 6]))

    @pl.when(col != place.chip)
    def _():
        row_copy(row_slot).start()

    @pl.when(owner)
    def _():
        r_kernel[my_slot] = own[pl.ds(col * per_owner, per_owner)]

    @pl.when(col == place.chip)
    def _():
        r_row[place.n_x + place.x] = own[kt + 3 : kt + 6]

    mix_maps(acts, mix_rows, mixb, contact)

    far_copy = remote(p_emb, y_emb, y_s.at[0], y_s.at[1], place.far, col)

    def z_copy(sems, buf, src, dst):
        return remote(buf.at[src], buf.at[src], sems.at[0, dst], sems.at[1, src], place.z_peer(dst), col)

    def kernel_in(slot):
        return remote(
            own.at[pl.ds(0, per_owner)], r_kernel.at[slot], kern_s.at[0, 0], kern_s.at[1, slot], row, col
        )

    @pl.when(owner)
    def _():
        for slot, (y, c) in enumerate(place.plane()):

            @pl.when(jnp.logical_not(place.is_me(y, c)))
            def _():
                kernel_in(slot).wait_recv()

        z_kernel[place.z] = b16(total(r_kernel, 2 * n_col))
        for dst in range(n_z):

            @pl.when(dst != place.z)
            def _():
                z_copy(zk_s, z_kernel, place.z, dst).start()

    mine = f32(own[kt : kt + 3])

    @pl.when(jnp.logical_not(exchange.main_src))
    def _():
        p_emb[...] = b16(mine)

    @pl.when(exchange.main_src)
    def _():
        for slot, wanted, _, _ in exchange.targets(exchange.main_y):

            @pl.when(wanted)
            def _():
                row_copy(slot).wait_recv()

        p_emb[...] = b16(mine + total(r_row, len(NEAR) * place.n_x))

    far_copy.start()

    def gather_copy(n, y, c):
        return remote(full.at[half, n], full.at[half, n], ag_s.at[0, y * n_col + c], ag_s.at[1, n], place.plane_row(y), c)

    @pl.when(owner)
    def _():
        for src in range(n_z):

            @pl.when(src != place.z)
            def _():
                z_copy(zk_s, z_kernel, src, place.z).wait_recv()

        full[half, col] = b16(total(z_kernel, n_z))
        for y, c in place.plane():

            @pl.when(jnp.logical_not(place.is_me(y, c)))
            def _():
                gather_copy(col, y, c).start()

    far_copy.wait()
    z_emb[place.z] = b16(f32(p_emb[...]) + f32(y_emb[...]))
    for dst in range(n_z):

        @pl.when(dst != place.z)
        def _():
            z_copy(ze_s, z_emb, place.z, dst).start()

    for src in range(n_z):

        @pl.when(src != place.z)
        def _():
            z_copy(ze_s, z_emb, src, place.z).wait_recv()

    emb_all[half] = b16(total(z_emb, n_z))
    emb_swap = remote(emb_all.at[half], emb_all.at[half], fin_s.at[0, 0], fin_s.at[1, 0], place.partner, col)
    emb_swap.start()
    to = col - 1 + 2 * half
    exists = (to >= 0) & (to < n_col)
    came = col + 1 - 2 * half
    came_ok = (came >= 0) & (came < n_col)

    def margin_copy(n, slot, device_row, device_col):
        return remote(
            emb_all.at[half, 2 * half], margins.at[slot],
            fin_s.at[0, 1 + n], fin_s.at[1, 1 + n], device_row, device_col,
        )

    @pl.when(exists)
    def _():
        margin_copy(0, half, row, to).start()
        margin_copy(1, half, place.partner, to).start()

    for n in range(owners):

        @pl.when(jnp.logical_not(place.is_me(n % 2, n)))
        def _():
            gather_copy(n, place.y, col).wait_recv()

    share = remote(full.at[half], full.at[half], agc_s.at[0], agc_s.at[1], place.partner, col)
    share.start()

    emb_swap.wait()

    @pl.when(came_ok)
    def _():
        margin_copy(0, half, row, col).wait_recv()

    @pl.when(exists)
    def _():
        margin_copy(1, 1 - half, row, col).wait_recv()

    main = [f32(emb_all[0, 1]), f32(emb_all[0, 2]), f32(emb_all[1, 0]), f32(emb_all[1, 1])]
    emb_out[0] = main[0] + f32(margins[1])
    emb_out[1] = main[1]
    emb_out[2] = main[2]
    emb_out[3] = main[3] + f32(margins[0])

    exchange.sent()
    for n in range(owners):

        @pl.when(jnp.logical_not(place.is_me(n % 2, n)))
        def _():
            kernel_copy(my_slot, n).wait_send()

    @pl.when(col != place.chip)
    def _():
        row_copy(row_slot).wait_send()

    for dst in range(n_z):

        @pl.when((dst != place.z) & owner)
        def _():
            z_copy(zk_s, z_kernel, place.z, dst).wait_send()

        @pl.when(dst != place.z)
        def _():
            z_copy(ze_s, z_emb, place.z, dst).wait_send()

    @pl.when(owner)
    def _():
        for y, c in place.plane():

            @pl.when(jnp.logical_not(place.is_me(y, c)))
            def _():
                gather_copy(col, y, c).wait_send()

    @pl.when(exists)
    def _():
        margin_copy(0, half, row, to).wait_send()
        margin_copy(1, half, place.partner, to).wait_send()

    share.wait()
    kernel_out[...] = full[...]


def fused_scratch(n_row, n_col, owners, per_owner, loaded):
    n_z = n_row // 4
    kt = owners * per_owner

    def tiles(*lead):
        return pltpu.VMEM((*lead, TILE, LANES), jnp.bfloat16)

    def sems(*shape):
        return pltpu.SemaphoreType.DMA(shape)

    return [
        tiles(4), tiles(6), tiles(2, kt + 6), tiles(kt + 6), tiles(kt + 6), tiles(2 * n_col, per_owner), tiles(4 * n_col // N_LO, 3),
        tiles(3), tiles(3), tiles(n_z, per_owner), tiles(n_z, 3), tiles(2, owners, per_owner), tiles(2, 3), tiles(2),
        sems(4 * n_col // N_LO), sems(4 * n_col // N_LO), sems(2), sems(4), sems(2, 2), sems(2, 2 * n_col), sems(1 + 4 * n_col // N_LO), sems(2),
        sems(2, n_z), sems(2, n_z), sems(2, 2 * n_col), sems(2), sems(2, 3),
        pltpu.SemaphoreType.REGULAR, *loaded, sems(len(loaded)),
    ]


def finish_kernel(per_owner, contact, grad, emb, contact_out, grad_out, emb_out):
    contact_out[...] = contact[...]
    emb_out[...] = emb[...]
    for k in range(grad_out.shape[0]):
        grad_out[k] = f32(grad[k % 2, k // (2 * per_owner), (k // 2) % per_owner])


def per_device(n_row, n_col, embedding, dilation, kernel, kernel_bias, mixing, mixing_bias, cotangent):
    channels = embedding.shape[1]
    filters = kernel.shape[2]
    maps, rows, cols = cotangent.shape
    bins = cols * n_col
    count = 9 * filters // TILE
    per_owner = -(-count // (2 * n_col))
    owners = -(-count // (2 * per_owner))
    loaded = [
        pltpu.VMEM((cols // TILE, TILE, channels), jnp.bfloat16),
        pltpu.SMEM((2,), jnp.int32),
        pltpu.VMEM(kernel.shape, jnp.bfloat16),
        pltpu.VMEM((1, filters), jnp.float32),
        pltpu.VMEM(mixing.shape, jnp.bfloat16),
        pltpu.SMEM((maps,), jnp.float32),
        pltpu.VMEM(cotangent.shape, jnp.bfloat16),
    ]
    contact, grad, emb = pl.pallas_call(
        functools.partial(fused_kernel, n_row, n_col, owners, per_owner, rows, cols, bins),
        out_shape=[
            jax.ShapeDtypeStruct((maps, rows, cols), jnp.float32),
            jax.ShapeDtypeStruct((2, owners, per_owner, TILE, channels), jnp.bfloat16),
            jax.ShapeDtypeStruct((cols // TILE, TILE, channels), jnp.float32),
        ],
        in_specs=[pl.BlockSpec(memory_space=pltpu.HBM)] * 7,
        out_specs=[VM, VM, VM],
        scratch_shapes=compute_scratch(rows, cols) + fused_scratch(n_row, n_col, owners, per_owner, loaded),
        compiler_params=pltpu.CompilerParams(collective_id=0, has_side_effects=True, vmem_limit_bytes=VMEM),
    )(
        *(
            pltpu.with_memory_space_constraint(value, pltpu.HBM)
            for value in (
                dilation,
                embedding.reshape(cols // TILE, TILE, channels),
                kernel,
                kernel_bias[None],
                mixing,
                mixing_bias,
                cotangent,
            )
        )
    )
    contact, grad, emb = pl.pallas_call(
        functools.partial(finish_kernel, per_owner),
        out_shape=[
            jax.ShapeDtypeStruct((maps, rows, cols), jnp.float32),
            jax.ShapeDtypeStruct((count, TILE, channels), jnp.float32),
            jax.ShapeDtypeStruct((cols // TILE, TILE, channels), jnp.float32),
        ],
        in_specs=[VM, VM, VM],
        out_specs=[VM, VM, VM],
        compiler_params=pltpu.CompilerParams(vmem_limit_bytes=VMEM),
    )(contact, grad, emb)
    return contact, emb.reshape(cols, channels), grad.reshape(3, 3, filters, channels)


def solution(mesh):
    return jax.shard_map(
        functools.partial(per_device, mesh.shape["row"], mesh.shape["col"]),
        mesh=mesh,
        in_specs=(P("col", None), P(), P(), P(), P(), P(), P(None, "row", "col")),
        out_specs=(P(None, "row", "col"), P("col", None), P()),
        check_vma=False,
    )
```
